256 devices in a mesh: scen: 64 (over z_hi, x, y, core), col: 4 (over z_lo).
Axes of the slice: x: 4, y: 4, z: 8 (z_hi: 2, z_lo: 4; z = z_hi * 4 + z_lo), core: 2. Of those that a mesh axis runs over, the one named last changes fastest.
Arguments:
- coef: float32 [32768, 8192], P('scen', 'col'), as said below
- mask: int32 [32768], replicated, may hold values from 0 to 1, as said below
- assign: int32 [4096], replicated, may hold values from 0 to 4095, each once
Outputs:
- master: float32 [4, 2048, 32768], P('col', 'scen')
The draws below stay inside these ranges and needn't reach their ends.
Inputs may be any that keep to these rules, and one draw needn't show every extreme that they name: `mask`: in each aligned block of 512 cuts (the cuts of one index of scen) exactly 256 are active. `coef`: magnitudes of rows and of columns differ widely; entries are finite and not zero on every row.
All inputs are finite; a program needn't handle non-finite values.
Results may differ from the reference program's by a relative error of at most 0.00007.
Values sent between devices are 32-bit elements; how exact they have to be, the bound alone decides.
A program may use at most 128 MiB of HBM per device.

```python
import jax
import jax.numpy as jnp
from jax import lax

NV = 8192
K = 8
SCEN_DEV = 64
ROWS_DEV = 512
ACT_DEV = 256
SCEN = 4096
CUTS = 32768
GROUPS = 4
N_SCEN = 64


def draw_coef(key, part):
    keys = jax.random.split(jax.random.fold_in(key, 11), 3)
    ramp = 1.0 + 2.0 * jnp.arange(NV, dtype=jnp.float32) / NV
    base = jax.random.normal(keys[0], (CUTS, NV), jnp.float32)
    row_scale = jnp.exp(jax.random.uniform(keys[1], (CUTS, 1), jnp.float32, -2.3, 2.3))
    col_scale = jnp.exp(jax.random.uniform(keys[2], (1, NV), jnp.float32, -2.3, 2.3)) * ramp[None, :]
    return (base * row_scale * col_scale).astype(jnp.float32)


def draw_mask(key, part):
    blocks = SCEN // SCEN_DEV
    keys = jax.random.split(jax.random.fold_in(key, 23), blocks)
    orders = jax.vmap(lambda sub: jax.random.permutation(sub, ROWS_DEV))(keys)
    return (orders < ACT_DEV).astype(jnp.int32).reshape(CUTS)


def setup_inputs(seed: int = 0) -> dict:
    streams_of = jax.random.split(jax.random.key(seed), 4)
    return {
        "coef": draw_coef(jax.random.fold_in(streams_of[3], 71), 0),
        "mask": draw_mask(jax.random.fold_in(streams_of[3], 71), 0),
        "assign": jax.random.permutation(streams_of[2], SCEN).astype(jnp.int32),
    }


EPS = 1e-06

def reference(coef, mask, assign):
    total = lax.optimization_barrier(jnp.sum(coef * coef, axis=1))
    row_norm = jnp.sqrt(total / NV + EPS)
    live = mask.astype(jnp.float32)
    scaled = coef / row_norm[:, None] * live[:, None]
    column = lax.optimization_barrier(jnp.sum(scaled * scaled, axis=0))
    col_norm = jnp.sqrt(column / (ACT_DEV * N_SCEN) + EPS)
    equil = scaled / col_norm[None, :]
    inverse = jnp.argsort(assign, stable=True).astype(jnp.int32)
    position = jnp.arange(CUTS, dtype=jnp.int32)
    source = inverse[position // K] * K + position % K
    master = jnp.take(equil, source, axis=0).T
    return master.reshape(GROUPS, NV // GROUPS, CUTS)
```

```python
import functools

import jax
import jax.numpy as jnp
from jax import lax
from jax.experimental import pallas as pl
from jax.experimental.pallas import tpu as pltpu
from jax.sharding import PartitionSpec as P

NV = 8192
K = 8
ACT_DEV = 256
EPS = 1e-06

LANES = 128
PART = 32
QROWS = 64
HELD = QROWS + 8
N_SCEN = 64
COLS = 4
MESH = pl.DeviceIdType.MESH
F32 = jnp.float32
BF16 = jnp.bfloat16


def iota(shape, dim):
    return lax.broadcasted_iota(jnp.int32, shape, dim)


def ones_where(cond):
    return jnp.where(cond, 1.0, 0.0).astype(BF16)


def dot(a, b):
    return jnp.dot(a, b, preferred_element_type=F32)


def dot_nt(a, b):
    return lax.dot_general(
        a, b, (((1,), (1,)), ((), ())), preferred_element_type=F32
    )


def exchange_kernel(
    coef_ref,
    mask_ref,
    assign_ref,
    held_ref,
    inv_ref,
    tbl_ref,
    idx_ref,
    val_ref,
    coef_v,
    pick,
    dense,
    packed,
    part,
    slots,
    in_sem,
    csend,
    crecv,
    zsem,
    ssem,
    rsem,
):
    rows, width = coef_ref.shape
    me = lax.axis_index("scen")
    group = lax.axis_index("col")
    half = N_SCEN // 2
    zh = me // half
    chunk = 256
    n_chunks = width // chunk

    def load(e):
        cols = pl.ds(pl.multiple_of(e * chunk, chunk), chunk)
        return pltpu.make_async_copy(
            coef_ref.at[:, cols], coef_v.at[:, cols], in_sem.at[e]
        )

    for e in range(n_chunks):
        load(e).start()

    barrier = pltpu.get_barrier_semaphore()
    across = (me + half) % N_SCEN
    pl.semaphore_signal(
        barrier, inc=1, device_id={"scen": across}, device_id_type=MESH
    )
    for d in range(1, COLS):
        pl.semaphore_signal(
            barrier,
            inc=1,
            device_id={"col": (group + d) % COLS},
            device_id_type=MESH,
        )

    def greet(t, _):
        pl.semaphore_signal(
            barrier,
            inc=1,
            device_id={"scen": zh * half + (me + t) % half},
            device_id_type=MESH,
        )
        return 0

    lax.fori_loop(1, half, greet, 0)

    own = mask_ref[pl.ds(pl.multiple_of(me // 2 * 8, 8), 8), :].astype(F32)
    own = jnp.where(me % 2 == 1, pltpu.roll(own, 4, 0), own)
    before = ones_where(iota((LANES, LANES), 0) < iota((LANES, LANES), 1))
    rank = dot(own.astype(BF16), before)
    base = jnp.zeros((1, 1), F32)
    for k in range(rows // LANES):
        row = own[k : k + 1, :]
        here = (rank[k : k + 1, :] + base).astype(jnp.int32)
        here = jnp.where(row > 0.5, here, -1)
        pick[:, k * LANES : (k + 1) * LANES] = ones_where(
            iota((ACT_DEV, LANES), 0) == here
        )
        base = base + jnp.sum(row, axis=1, keepdims=True)

    def compact(e, acc):
        load(e).wait()
        cols = pl.ds(pl.multiple_of(e * chunk, chunk), chunk)
        x = coef_v[:, cols]
        hi = x.astype(BF16)
        rest = x - hi.astype(F32)
        mid = rest.astype(BF16)
        low = (rest - mid.astype(F32)).astype(BF16)
        sel = pick[...]
        z = dot(sel, hi) + dot(sel, mid) + dot(sel, low)
        dense[:, cols] = z
        for j in range(chunk // LANES):
            zj = z[:, j * LANES : (j + 1) * LANES]
            acc = acc + zj * zj
        return acc

    acc = lax.fori_loop(0, n_chunks, compact, jnp.zeros((ACT_DEV, LANES), F32))
    mine = jnp.sum(acc.T, axis=0, keepdims=True)
    part[group] = jnp.broadcast_to(mine, (8, ACT_DEV))

    pl.semaphore_wait(barrier, half - 1 + 1 + COLS - 1)

    def share(d):
        return pltpu.make_async_remote_copy(
            src_ref=part.at[group],
            dst_ref=part.at[group],
            send_sem=csend.at[d - 1],
            recv_sem=crecv.at[d - 1],
            device_id={"col": (group + d) % COLS},
            device_id_type=MESH,
        )

    for d in range(1, COLS):
        share(d).start()
    pl.semaphore_signal(zsem, inc=1, device_id={"scen": across}, device_id_type=MESH)
    for d in range(1, COLS):
        share(d).wait()
    total = part[0] + part[1] + part[2] + part[3]
    inv_row = 1.0 / jnp.sqrt(total[0:1, :] / NV + EPS)
    scale = jnp.broadcast_to(inv_row, (LANES, ACT_DEV)).T
    pl.semaphore_wait(zsem, 1)

    lane_group = iota((QROWS, LANES), 1) // PART

    def send(d):
        return pltpu.make_async_remote_copy(
            src_ref=packed.at[d],
            dst_ref=held_ref.at[me],
            send_sem=ssem.at[d],
            recv_sem=rsem.at[me],
            device_id={"scen": d},
            device_id_type=MESH,
        )

    n_tiles = width // LANES
    half_tiles = n_tiles // 2
    own_tile = (me % half) // 4

    def pack(i, _):
        e = ((1 - zh + i // half_tiles) % 2) * half_tiles + (own_tile + i) % half_tiles
        cols = pl.ds(pl.multiple_of(e * LANES, LANES), LANES)
        quarters = [
            dense[q * QROWS : (q + 1) * QROWS, cols]
            * scale[q * QROWS : (q + 1) * QROWS, :]
            for q in range(4)
        ]
        for f in range(4):
            out = None
            for q in range(4):
                shift = PART * (q - f) % LANES
                moved = pltpu.roll(quarters[q], shift, 1) if shift else quarters[q]
                out = moved if out is None else jnp.where(lane_group == q, moved, out)
            packed[4 * e + f] = out
        for f in range(4):
            d = 4 * e + (f + me) % 4

            @pl.when(d != me)
            def _():
                send(d).start()

        return 0

    lax.fori_loop(0, n_tiles, pack, 0)
    held_ref[me] = packed[me]

    count = jnp.zeros((32, LANES), F32)
    bits = jnp.zeros((32, LANES), F32)
    r_i, l_i = iota((LANES, LANES), 0), iota((LANES, LANES), 1)
    for a in range(8):
        m = mask_ref[pl.ds(a, 32, stride=8), :].astype(F32).astype(BF16)
        pool = jnp.where(l_i == 16 * a + r_i // K, 1.0, 0.0)
        weight = lax.shift_left(jnp.ones_like(r_i), r_i % K).astype(F32)
        count = count + dot(m, pool.astype(BF16))
        bits = bits + dot(m, (pool * weight).astype(BF16))
    first = dot(
        count.astype(BF16), ones_where((r_i < l_i) & (r_i // 64 == l_i // 64))
    ).astype(jnp.int32)
    to = assign_ref[...]
    source = 2 * iota((32, LANES), 0) + iota((32, LANES), 1) // 64
    quarter = lax.rem(lax.rem(to, 64) // 16 - first // QROWS + 8, 4)
    at = quarter * (N_SCEN * HELD) + source * HELD + lax.rem(first, QROWS)
    slots[0] = (to // 64).astype(F32)
    slots[1] = lax.rem(to, 64).astype(F32)
    slots[2] = (at // 256).astype(F32)
    slots[3] = lax.rem(at, 256).astype(F32)
    slots[4] = bits

    def place(k, acc):
        s_i = iota((64, LANES), 0).astype(F32)
        high = jnp.where(s_i == slots[0, pl.ds(k, 1), :], 1.0, 0.0)
        low = jnp.where(s_i == slots[1, pl.ds(k, 1), :], 1.0, 0.0).astype(BF16)
        return tuple(
            acc[j] + dot_nt((high * slots[2 + j, pl.ds(k, 1), :]).astype(BF16), low)
            for j in range(3)
        )

    zero = jnp.zeros((64, 64), F32)
    at_hi, at_lo, pattern = lax.fori_loop(0, 32, place, (zero, zero, zero))
    tbl_ref[...] = (at_hi * 256.0 + at_lo).astype(jnp.int32)
    k_i = lax.rem(iota((64, LANES), 1), K)
    for q in range(4):
        spread = ones_where(iota((64, LANES), 0) - 16 * q == iota((64, LANES), 1) // K)
        pat = dot(pattern.astype(BF16), spread).astype(jnp.int32)
        before_k = jnp.zeros((64, LANES), jnp.int32)
        own_bit = jnp.zeros((64, LANES), jnp.int32)
        for m in range(K):
            bit = lax.shift_right_logical(pat, m) & 1
            before_k = before_k + jnp.where(k_i > m, bit, 0)
            own_bit = own_bit + jnp.where(k_i == m, bit, 0)
        idx_ref[q] = iota((64, LANES), 1) - k_i + before_k
        val_ref[q] = own_bit.astype(F32)

    def take(t, acc):
        s = (me + t) % N_SCEN

        @pl.when(t > 0)
        def _():
            pltpu.make_async_remote_copy(
                src_ref=packed.at[s],
                dst_ref=held_ref.at[s],
                send_sem=ssem.at[s],
                recv_sem=rsem.at[s],
                device_id={"scen": s},
                device_id_type=MESH,
            ).wait_recv()

        x = held_ref[s]
        return acc + x * x

    acc = lax.fori_loop(0, N_SCEN, take, jnp.zeros((QROWS, LANES), F32))
    col = jnp.sum(acc, axis=0, keepdims=True)
    col = jnp.broadcast_to(col, (8, LANES))
    col = col + pltpu.roll(col, 64, 1)
    col = col + pltpu.roll(col, 32, 1)
    inv_ref[...] = 1.0 / jnp.sqrt(col / (ACT_DEV * N_SCEN) + EPS)

    def finish(t, _):
        d = (me + t) % N_SCEN

        send(d).wait_send()
        return 0

    lax.fori_loop(1, N_SCEN, finish, 0)


def place_kernel(per_step, tbl_ref, held_ref, inv_ref, idx_ref, val_ref, out_ref, turned):
    step = pl.program_id(0)

    @pl.when(step == 0)
    def _():
        inv = jnp.broadcast_to(inv_ref[0:1, :], (HELD, LANES))

        def turn(s, _):
            x = held_ref[s]
            x = jnp.concatenate([x, pltpu.roll(x[:8], LANES - PART, 1)], axis=0) * inv
            for p in range(4):
                y = pltpu.roll(x, PART * p, 1) if p else x
                turned[pl.ds(pl.multiple_of((p * N_SCEN + s) * HELD, 8), HELD), :] = y
            return 0

        lax.fori_loop(0, N_SCEN, turn, 0)

    lane_group = iota((8, LANES), 1) // PART

    def block(h, _):
        hi = step * per_step + h
        tiles = []
        for i in range(16):
            m = None
            for q in range(4):
                x = turned[pl.ds(tbl_ref[hi, 16 * q + i], 8), :]
                m = x if m is None else jnp.where(lane_group == q, x, m)
            tiles.append(m)
        flipped = jnp.concatenate(tiles, axis=0).T
        for q in range(4):
            idx = jnp.broadcast_to(idx_ref[q, pl.ds(hi, 1), :], (PART, LANES))
            val = jnp.broadcast_to(val_ref[q, pl.ds(hi, 1), :], (PART, LANES))
            y = flipped[q * PART : (q + 1) * PART, :]
            y = jnp.take_along_axis(y, idx, axis=1) * val
            out_ref[0, :, pl.ds(pl.multiple_of(h * 512 + q * LANES, LANES), LANES)] = y
        return 0

    lax.fori_loop(0, per_step, block, 0)


def on_device(coef, mask, assign):
    rows, width = coef.shape
    vmem = pl.BlockSpec(memory_space=pltpu.VMEM)
    held, inv, tbl, idx, val = pl.pallas_call(
        exchange_kernel,
        out_shape=(
            jax.ShapeDtypeStruct((N_SCEN, QROWS, LANES), F32),
            jax.ShapeDtypeStruct((8, LANES), F32),
            jax.ShapeDtypeStruct((64, 64), jnp.int32),
            jax.ShapeDtypeStruct((4, 64, LANES), jnp.int32),
            jax.ShapeDtypeStruct((4, 64, LANES), F32),
        ),
        in_specs=[pl.BlockSpec(memory_space=pltpu.HBM), vmem, vmem],
        out_specs=(vmem, vmem, vmem, vmem, vmem),
        scratch_shapes=[
            pltpu.VMEM((rows, width), F32),
            pltpu.VMEM((ACT_DEV, rows), BF16),
            pltpu.VMEM((ACT_DEV, width), F32),
            pltpu.VMEM((N_SCEN, QROWS, LANES), F32),
            pltpu.VMEM((COLS, 8, ACT_DEV), F32),
            pltpu.VMEM((5, 32, LANES), F32),
            pltpu.SemaphoreType.DMA((8,)),
            pltpu.SemaphoreType.DMA((COLS - 1,)),
            pltpu.SemaphoreType.DMA((COLS - 1,)),
            pltpu.SemaphoreType.REGULAR,
            pltpu.SemaphoreType.DMA((N_SCEN,)),
            pltpu.SemaphoreType.DMA((N_SCEN,)),
        ],
        compiler_params=pltpu.CompilerParams(
            collective_id=0, has_side_effects=True, vmem_limit_bytes=32 * 2**20
        ),
        name="exchange",
    )(coef, mask.reshape(256, LANES), assign.reshape(32, LANES))

    steps = 8
    per_step = 64 // steps

    def fixed(*shape):
        return pl.BlockSpec(shape, lambda i: (0,) * len(shape))

    return pl.pallas_call(
        functools.partial(place_kernel, per_step),
        out_shape=jax.ShapeDtypeStruct((1, PART, 64 * 512), F32),
        grid=(steps,),
        in_specs=[
            pl.BlockSpec(memory_space=pltpu.SMEM),
            fixed(N_SCEN, QROWS, LANES),
            fixed(8, LANES),
            fixed(4, 64, LANES),
            fixed(4, 64, LANES),
        ],
        out_specs=pl.BlockSpec((1, PART, per_step * 512), lambda i: (0, 0, i)),
        scratch_shapes=[pltpu.VMEM((4 * N_SCEN * HELD, LANES), F32)],
        compiler_params=pltpu.CompilerParams(
            dimension_semantics=("arbitrary",), vmem_limit_bytes=32 * 2**20
        ),
        name="place",
    )(tbl, held, inv, idx, val)


def solution(mesh):
    in_specs = (P("scen", "col"), P(), P())
    out_specs = P("col", "scen", None)
    return jax.shard_map(
        on_device, mesh=mesh, in_specs=in_specs, out_specs=out_specs, check_vma=False
    )
```

```python
import functools

import jax
import jax.numpy as jnp
from jax import lax
from jax.experimental import pallas as pl
from jax.experimental.pallas import tpu as pltpu
from jax.sharding import PartitionSpec as P

NV = 8192
K = 8
ACT_DEV = 256
EPS = 1e-06

LANES = 128
PART = 32
QROWS = 64
HELD = QROWS + 8
N_SCEN = 64
COLS = 4
MESH = pl.DeviceIdType.MESH
F32 = jnp.float32
BF16 = jnp.bfloat16


def iota(shape, dim):
    return lax.broadcasted_iota(jnp.int32, shape, dim)


def ones_where(cond):
    return jnp.where(cond, 1.0, 0.0).astype(BF16)


def dot(a, b):
    return jnp.dot(a, b, preferred_element_type=F32)


def dot_nt(a, b):
    return lax.dot_general(
        a, b, (((1,), (1,)), ((), ())), preferred_element_type=F32
    )


def exchange_kernel(
    coef_ref,
    mask_hbm,
    assign_hbm,
    turned,
    inv_ref,
    tbl_ref,
    idx_ref,
    val_ref,
    coef_v,
    mask_ref,
    assign_ref,
    pick,
    dense,
    packed,
    recv,
    part,
    slots,
    small_sem,
    in_sem,
    csend,
    crecv,
    zsem,
    ssem,
    rsem,
):
    rows, width = coef_ref.shape
    me = lax.axis_index("scen")
    group = lax.axis_index("col")
    half = N_SCEN // 2
    zh = me // half
    chunk = 256
    n_chunks = width // chunk

    def load(e):
        cols = pl.ds(pl.multiple_of(e * chunk, chunk), chunk)
        return pltpu.make_async_copy(
            coef_ref.at[:, cols], coef_v.at[:, cols], in_sem.at[e]
        )

    load_mask = pltpu.make_async_copy(mask_hbm, mask_ref, small_sem.at[0])
    load_assign = pltpu.make_async_copy(assign_hbm, assign_ref, small_sem.at[1])
    load_mask.start()
    for e in range(n_chunks):
        load(e).start()
    load_assign.start()

    barrier = pltpu.get_barrier_semaphore()
    across = (me + half) % N_SCEN
    pl.semaphore_signal(
        barrier, inc=1, device_id={"scen": across}, device_id_type=MESH
    )
    for d in range(1, COLS):
        pl.semaphore_signal(
            barrier,
            inc=1,
            device_id={"col": (group + d) % COLS},
            device_id_type=MESH,
        )

    def greet(t, _):
        pl.semaphore_signal(
            barrier,
            inc=1,
            device_id={"scen": zh * half + (me + t) % half},
            device_id_type=MESH,
        )
        return 0

    lax.fori_loop(1, half, greet, 0)

    load_mask.wait()

    own = mask_ref[pl.ds(pl.multiple_of(me // 2 * 8, 8), 8), :].astype(F32)
    own = jnp.where(me % 2 == 1, pltpu.roll(own, 4, 0), own)
    before = ones_where(iota((LANES, LANES), 0) < iota((LANES, LANES), 1))
    rank = dot(own.astype(BF16), before)
    base = jnp.zeros((1, 1), F32)
    for k in range(rows // LANES):
        row = own[k : k + 1, :]
        here = (rank[k : k + 1, :] + base).astype(jnp.int32)
        here = jnp.where(row > 0.5, here, -1)
        pick[:, k * LANES : (k + 1) * LANES] = ones_where(
            iota((ACT_DEV, LANES), 0) == here
        )
        base = base + jnp.sum(row, axis=1, keepdims=True)

    def compact(e, acc):
        load(e).wait()
        cols = pl.ds(pl.multiple_of(e * chunk, chunk), chunk)
        x = coef_v[:, cols]
        hi = x.astype(BF16)
        rest = x - hi.astype(F32)
        mid = rest.astype(BF16)
        low = (rest - mid.astype(F32)).astype(BF16)
        sel = pick[...]
        z = dot(sel, hi) + dot(sel, mid) + dot(sel, low)
        dense[:, cols] = z
        for j in range(chunk // LANES):
            zj = z[:, j * LANES : (j + 1) * LANES]
            acc = acc + zj * zj
        return acc

    acc = lax.fori_loop(0, n_chunks, compact, jnp.zeros((ACT_DEV, LANES), F32))
    mine = jnp.sum(acc.T, axis=0, keepdims=True)
    part[group] = jnp.broadcast_to(mine, (8, ACT_DEV))

    pl.semaphore_wait(barrier, half - 1 + 1 + COLS - 1)

    def share(d):
        return pltpu.make_async_remote_copy(
            src_ref=part.at[group],
            dst_ref=part.at[group],
            send_sem=csend.at[d - 1],
            recv_sem=crecv.at[d - 1],
            device_id={"col": (group + d) % COLS},
            device_id_type=MESH,
        )

    for d in range(1, COLS):
        share(d).start()
    pl.semaphore_signal(zsem, inc=1, device_id={"scen": across}, device_id_type=MESH)
    for d in range(1, COLS):
        share(d).wait()
    total = part[0] + part[1] + part[2] + part[3]
    inv_row = 1.0 / jnp.sqrt(total[0:1, :] / NV + EPS)
    scale = jnp.broadcast_to(inv_row, (LANES, ACT_DEV)).T
    pl.semaphore_wait(zsem, 1)

    lane_group = iota((QROWS, LANES), 1) // PART

    def send(d):
        return pltpu.make_async_remote_copy(
            src_ref=packed.at[d],
            dst_ref=recv.at[me],
            send_sem=ssem.at[d],
            recv_sem=rsem.at[me],
            device_id={"scen": d},
            device_id_type=MESH,
        )

    n_tiles = width // LANES
    half_tiles = n_tiles // 2
    own_tile = (me % half) // 4

    def pack(i, _):
        e = ((1 - zh + i // half_tiles) % 2) * half_tiles + (own_tile + i) % half_tiles
        cols = pl.ds(pl.multiple_of(e * LANES, LANES), LANES)
        quarters = [
            dense[q * QROWS : (q + 1) * QROWS, cols]
            * scale[q * QROWS : (q + 1) * QROWS, :]
            for q in range(4)
        ]
        for f in range(4):
            out = None
            for q in range(4):
                shift = PART * (q - f) % LANES
                moved = pltpu.roll(quarters[q], shift, 1) if shift else quarters[q]
                out = moved if out is None else jnp.where(lane_group == q, moved, out)
            packed[4 * e + f] = out
        for f in range(4):
            d = 4 * e + (f + me) % 4

            @pl.when(d != me)
            def _():
                send(d).start()

        return 0

    lax.fori_loop(0, n_tiles, pack, 0)
    recv[me] = packed[me]

    count = jnp.zeros((32, LANES), F32)
    bits = jnp.zeros((32, LANES), F32)
    r_i, l_i = iota((LANES, LANES), 0), iota((LANES, LANES), 1)
    for a in range(8):
        m = mask_ref[pl.ds(a, 32, stride=8), :].astype(F32).astype(BF16)
        pool = jnp.where(l_i == 16 * a + r_i // K, 1.0, 0.0)
        weight = lax.shift_left(jnp.ones_like(r_i), r_i % K).astype(F32)
        count = count + dot(m, pool.astype(BF16))
        bits = bits + dot(m, (pool * weight).astype(BF16))
    first = dot(
        count.astype(BF16), ones_where((r_i < l_i) & (r_i // 64 == l_i // 64))
    ).astype(jnp.int32)
    load_assign.wait()
    to = assign_ref[...]
    source = 2 * iota((32, LANES), 0) + iota((32, LANES), 1) // 64
    quarter = lax.rem(lax.rem(to, 64) // 16 - first // QROWS + 8, 4)
    at = quarter * (N_SCEN * HELD) + source * HELD + lax.rem(first, QROWS)
    slots[0] = (to // 64).astype(F32)
    slots[1] = lax.rem(to, 64).astype(F32)
    slots[2] = (at // 256).astype(F32)
    slots[3] = lax.rem(at, 256).astype(F32)
    slots[4] = bits

    def place(k, acc):
        s_i = iota((64, LANES), 0).astype(F32)
        high = jnp.where(s_i == slots[0, pl.ds(k, 1), :], 1.0, 0.0)
        low = jnp.where(s_i == slots[1, pl.ds(k, 1), :], 1.0, 0.0).astype(BF16)
        return tuple(
            acc[j] + dot_nt((high * slots[2 + j, pl.ds(k, 1), :]).astype(BF16), low)
            for j in range(3)
        )

    zero = jnp.zeros((64, 64), F32)
    at_hi, at_lo, pattern = lax.fori_loop(0, 32, place, (zero, zero, zero))
    tbl_ref[...] = (at_hi * 256.0 + at_lo).astype(jnp.int32)
    k_i = lax.rem(iota((64, LANES), 1), K)
    for q in range(4):
        spread = ones_where(iota((64, LANES), 0) - 16 * q == iota((64, LANES), 1) // K)
        pat = dot(pattern.astype(BF16), spread).astype(jnp.int32)
        before_k = jnp.zeros((64, LANES), jnp.int32)
        own_bit = jnp.zeros((64, LANES), jnp.int32)
        for m in range(K):
            bit = lax.shift_right_logical(pat, m) & 1
            before_k = before_k + jnp.where(k_i > m, bit, 0)
            own_bit = own_bit + jnp.where(k_i == m, bit, 0)
        idx_ref[q] = iota((64, LANES), 1) - k_i + before_k
        val_ref[q] = own_bit.astype(F32)

    def take(t, acc):
        s = (me + t) % N_SCEN

        @pl.when(t > 0)
        def _():
            pltpu.make_async_remote_copy(
                src_ref=packed.at[s],
                dst_ref=recv.at[s],
                send_sem=ssem.at[s],
                recv_sem=rsem.at[s],
                device_id={"scen": s},
                device_id_type=MESH,
            ).wait_recv()

        x = recv[s]
        tall = jnp.concatenate([x, pltpu.roll(x[:8], LANES - PART, 1)], axis=0)
        for p in range(4):
            y = pltpu.roll(tall, PART * p, 1) if p else tall
            turned[pl.ds(pl.multiple_of((p * N_SCEN + s) * HELD, 8), HELD), :] = y
        return acc + x * x

    acc = lax.fori_loop(0, N_SCEN, take, jnp.zeros((QROWS, LANES), F32))
    col = jnp.sum(acc, axis=0, keepdims=True)
    col = jnp.broadcast_to(col, (8, LANES))
    col = col + pltpu.roll(col, 64, 1)
    col = col + pltpu.roll(col, 32, 1)
    inv_ref[...] = 1.0 / jnp.sqrt(col / (ACT_DEV * N_SCEN) + EPS)

    def finish(t, _):
        d = (me + t) % N_SCEN

        send(d).wait_send()
        return 0

    lax.fori_loop(1, N_SCEN, finish, 0)


def place_kernel(per_step, tbl_ref, turned, inv_ref, idx_ref, val_ref, out_ref):
    step = pl.program_id(0)
    inv = inv_ref[...]
    lane_group = iota((8, LANES), 1) // PART

    for h in range(per_step):
        hi = step * per_step + h
        tiles = []
        for i in range(16):
            m = None
            for q in range(4):
                x = turned[pl.ds(tbl_ref[hi, 16 * q + i], 8), :]
                m = x if m is None else jnp.where(lane_group == q, x, m)
            tiles.append(m * inv)
        flipped = jnp.concatenate(tiles, axis=0).T
        for q in range(4):
            idx = jnp.broadcast_to(idx_ref[q, pl.ds(hi, 1), :], (PART, LANES))
            val = jnp.broadcast_to(val_ref[q, pl.ds(hi, 1), :], (PART, LANES))
            y = flipped[q * PART : (q + 1) * PART, :]
            y = jnp.take_along_axis(y, idx, axis=1) * val
            at = h * 512 + q * LANES
            out_ref[0, :, at : at + LANES] = y


def on_device(coef, mask, assign):
    rows, width = coef.shape
    vmem = pl.BlockSpec(memory_space=pltpu.VMEM)
    hbm = pl.BlockSpec(memory_space=pltpu.HBM)

    def in_hbm(x):
        return pltpu.with_memory_space_constraint(x, pltpu.HBM)

    turned, inv, tbl, idx, val = pl.pallas_call(
        exchange_kernel,
        out_shape=(
            pltpu.VMEM((4 * N_SCEN * HELD, LANES), F32),
            jax.ShapeDtypeStruct((8, LANES), F32),
            jax.ShapeDtypeStruct((64, 64), jnp.int32),
            jax.ShapeDtypeStruct((4, 64, LANES), jnp.int32),
            jax.ShapeDtypeStruct((4, 64, LANES), F32),
        ),
        in_specs=[hbm, hbm, hbm],
        out_specs=(vmem, vmem, vmem, vmem, vmem),
        scratch_shapes=[
            pltpu.VMEM((rows, width), F32),
            pltpu.VMEM((256, LANES), jnp.int32),
            pltpu.VMEM((32, LANES), jnp.int32),
            pltpu.VMEM((ACT_DEV, rows), BF16),
            pltpu.VMEM((ACT_DEV, width), F32),
            pltpu.VMEM((N_SCEN, QROWS, LANES), F32),
            pltpu.VMEM((N_SCEN, QROWS, LANES), F32),
            pltpu.VMEM((COLS, 8, ACT_DEV), F32),
            pltpu.VMEM((5, 32, LANES), F32),
            pltpu.SemaphoreType.DMA((2,)),
            pltpu.SemaphoreType.DMA((8,)),
            pltpu.SemaphoreType.DMA((COLS - 1,)),
            pltpu.SemaphoreType.DMA((COLS - 1,)),
            pltpu.SemaphoreType.REGULAR,
            pltpu.SemaphoreType.DMA((N_SCEN,)),
            pltpu.SemaphoreType.DMA((N_SCEN,)),
        ],
        compiler_params=pltpu.CompilerParams(
            collective_id=0, has_side_effects=True, vmem_limit_bytes=20 * 2**20
        ),
        name="exchange",
    )(
        in_hbm(coef),
        in_hbm(mask.reshape(256, LANES)),
        in_hbm(assign.reshape(32, LANES)),
    )

    steps = 8
    per_step = 64 // steps

    def fixed(*shape):
        return pl.BlockSpec(shape, lambda i: (0,) * len(shape))

    return pl.pallas_call(
        functools.partial(place_kernel, per_step),
        out_shape=jax.ShapeDtypeStruct((1, PART, 64 * 512), F32),
        grid=(steps,),
        in_specs=[
            pl.BlockSpec(memory_space=pltpu.SMEM),
            vmem,
            fixed(8, LANES),
            fixed(4, 64, LANES),
            fixed(4, 64, LANES),
        ],
        out_specs=pl.BlockSpec((1, PART, per_step * 512), lambda i: (0, 0, i)),
        compiler_params=pltpu.CompilerParams(
            dimension_semantics=("arbitrary",), vmem_limit_bytes=16 * 2**20
        ),
        name="place",
    )(tbl, turned, inv, idx, val)


def solution(mesh):
    in_specs = (P("scen", "col"), P(), P())
    out_specs = P("col", "scen", None)
    return jax.shard_map(
        on_device, mesh=mesh, in_specs=in_specs, out_specs=out_specs, check_vma=False
    )
```

```python
import functools

import jax
import jax.numpy as jnp
from jax import lax
from jax.experimental import pallas as pl
from jax.experimental.pallas import tpu as pltpu
from jax.sharding import PartitionSpec as P

NV = 8192
K = 8
ACT_DEV = 256
EPS = 1e-06

LANES = 128
PART = 32
QROWS = 64
HELD = QROWS + 8
N_SCEN = 64
LAG = 4
COLS = 4
MESH = pl.DeviceIdType.MESH
F32 = jnp.float32
BF16 = jnp.bfloat16


def iota(shape, dim):
    return lax.broadcasted_iota(jnp.int32, shape, dim)


def ones_where(cond):
    return jnp.where(cond, 1.0, 0.0).astype(BF16)


def dot(a, b):
    return jnp.dot(a, b, preferred_element_type=F32)


def dot_nt(a, b):
    return lax.dot_general(
        a, b, (((1,), (1,)), ((), ())), preferred_element_type=F32
    )


def exchange_kernel(
    coef_ref,
    mask_hbm,
    assign_hbm,
    turned,
    inv_ref,
    tbl_ref,
    idx_ref,
    val_ref,
    coef_v,
    mask_ref,
    assign_ref,
    pick,
    dense,
    packed,
    relay,
    recv,
    part,
    slots,
    small_sem,
    in_sem,
    csend,
    crecv,
    axis_sem,
    twin_sem,
    ssem,
    rsem,
    relay_sem,
    forward_sem,
):
    rows, width = coef_ref.shape
    me = lax.axis_index("scen")
    group = lax.axis_index("col")
    half = N_SCEN // 2
    zh = me // half
    chunk = 256
    n_chunks = width // chunk

    def load(e):
        cols = pl.ds(pl.multiple_of(e * chunk, chunk), chunk)
        return pltpu.make_async_copy(
            coef_ref.at[:, cols], coef_v.at[:, cols], in_sem.at[e]
        )

    load_mask = pltpu.make_async_copy(mask_hbm, mask_ref, small_sem.at[0])
    load_assign = pltpu.make_async_copy(assign_hbm, assign_ref, small_sem.at[1])
    load_mask.start()
    for e in range(n_chunks):
        load(e).start()
    load_assign.start()

    own = me % half
    across = (me + half) % N_SCEN
    own_x, own_y, own_c = own // 8, own // 2 % 4, own % 2

    def index(x, y, c):
        return x % 4 * 8 + y % 4 * 2 + c % 2

    def signal(sem, device):
        pl.semaphore_signal(sem, inc=1, device_id=device, device_id_type=MESH)

    along_x = [{"scen": zh * half + index(own_x + d, own_y, own_c)} for d in (1, 2, 3)]
    along_y = [{"scen": zh * half + index(own_x, own_y + d, own_c)} for d in (1, 2, 3)]
    twin = {"scen": zh * half + index(own_x, own_y, own_c + 1)}
    others = [{"col": (group + d) % COLS} for d in range(1, COLS)]

    barrier = pltpu.get_barrier_semaphore()
    for device in [{"scen": across}] + others + along_x + along_y + [twin]:
        signal(barrier, device)

    load_mask.wait()

    mine = mask_ref[pl.ds(pl.multiple_of(me // 2 * 8, 8), 8), :].astype(F32)
    mine = jnp.where(me % 2 == 1, pltpu.roll(mine, 4, 0), mine)
    before = ones_where(iota((LANES, LANES), 0) < iota((LANES, LANES), 1))
    rank = dot(mine.astype(BF16), before)
    base = jnp.zeros((1, 1), F32)
    for k in range(rows // LANES):
        row = mine[k : k + 1, :]
        here = (rank[k : k + 1, :] + base).astype(jnp.int32)
        here = jnp.where(row > 0.5, here, -1)
        pick[:, k * LANES : (k + 1) * LANES] = ones_where(
            iota((ACT_DEV, LANES), 0) == here
        )
        base = base + jnp.sum(row, axis=1, keepdims=True)

    def compact(e, acc):
        load(e).wait()
        cols = pl.ds(pl.multiple_of(e * chunk, chunk), chunk)
        x = coef_v[:, cols]
        hi = x.astype(BF16)
        rest = x - hi.astype(F32)
        mid = rest.astype(BF16)
        low = (rest - mid.astype(F32)).astype(BF16)
        sel = pick[...]
        z = dot(sel, hi) + dot(sel, mid) + dot(sel, low)
        dense[:, cols] = z
        for j in range(chunk // LANES):
            zj = z[:, j * LANES : (j + 1) * LANES]
            acc = acc + zj * zj
        return acc

    acc = lax.fori_loop(0, n_chunks, compact, jnp.zeros((ACT_DEV, LANES), F32))
    sums = jnp.sum(acc.T, axis=0, keepdims=True)
    part[group] = jnp.broadcast_to(sums, (8, ACT_DEV))

    pl.semaphore_wait(barrier, 11)

    def share(d):
        return pltpu.make_async_remote_copy(
            src_ref=part.at[group],
            dst_ref=part.at[group],
            send_sem=csend.at[d - 1],
            recv_sem=crecv.at[d - 1],
            device_id={"col": (group + d) % COLS},
            device_id_type=MESH,
        )

    for d in range(1, COLS):
        share(d).start()
    for device in along_x + [twin]:
        signal(axis_sem, device)
    for d in range(1, COLS):
        share(d).wait()
    total = part[0] + part[1] + part[2] + part[3]
    inv_row = 1.0 / jnp.sqrt(total[0:1, :] / NV + EPS)
    scale = jnp.broadcast_to(inv_row, (LANES, ACT_DEV)).T

    lane_group = iota((QROWS, LANES), 1) // PART

    def pack(e):
        cols = pl.ds(pl.multiple_of(e * LANES, LANES), LANES)
        quarters = [
            dense[q * QROWS : (q + 1) * QROWS, cols]
            * scale[q * QROWS : (q + 1) * QROWS, :]
            for q in range(4)
        ]
        for f in range(4):
            out = None
            for q in range(4):
                shift = PART * (q - f) % LANES
                moved = pltpu.roll(quarters[q], shift, 1) if shift else quarters[q]
                out = moved if out is None else jnp.where(lane_group == q, moved, out)
            packed[4 * e + f] = out

    def offset(i):
        late = i // 2
        return (1 - late) * (2 - i) + late * (9 - 3 * i)

    def ahead(k):
        return index(
            own_x + offset(k // 8), own_y + offset(k // 2 % 4), own_c + 1 - k % 2
        )

    def behind(k):
        return index(
            own_x + 4 - offset(k // 8), own_y + 4 - offset(k // 2 % 4), own_c + 1 - k % 2
        )

    def to_relay(j):
        return pltpu.make_async_remote_copy(
            src_ref=packed.at[(1 - zh) * half + j],
            dst_ref=relay.at[j],
            send_sem=ssem.at[(1 - zh) * half + j],
            recv_sem=relay_sem.at[j],
            device_id={"scen": across},
            device_id_type=MESH,
        )

    def direct(d):
        return pltpu.make_async_remote_copy(
            src_ref=packed.at[d],
            dst_ref=recv.at[me],
            send_sem=ssem.at[d],
            recv_sem=rsem.at[me],
            device_id={"scen": d},
            device_id_type=MESH,
        )

    def forward(j):
        return pltpu.make_async_remote_copy(
            src_ref=relay.at[j],
            dst_ref=recv.at[across],
            send_sem=forward_sem.at[j],
            recv_sem=rsem.at[across],
            device_id={"scen": zh * half + j},
            device_id_type=MESH,
        )

    def arrival(s):
        return pltpu.make_async_remote_copy(
            src_ref=packed.at[s],
            dst_ref=recv.at[s],
            send_sem=ssem.at[s],
            recv_sem=rsem.at[s],
            device_id={"scen": s},
            device_id_type=MESH,
        )

    last = half - 1

    def send_far(i, _):
        x = (own_x + offset(i)) % 4
        for p in range(2):
            pack((1 - zh) * 8 + x * 2 + p)
        for j in range(8):
            k = 8 * i + j
            if j < 7:
                to_relay(ahead(k)).start()
            else:

                @pl.when(k < last)
                def _():
                    to_relay(ahead(k)).start()

        return 0

    lax.fori_loop(0, 4, send_far, 0)
    direct(across).start()

    pl.semaphore_wait(axis_sem, 4)
    signal(twin_sem, twin)
    pl.semaphore_wait(twin_sem, 1)

    def send_near(i, _):
        x = (own_x + offset(i)) % 4
        for p in range(2):
            pack(zh * 8 + x * 2 + p)
        for j in range(8):
            k = 8 * i + j
            if j < 7:
                direct(zh * half + ahead(k)).start()
            else:

                @pl.when(k < last)
                def _():
                    direct(zh * half + ahead(k)).start()

        return 0

    lax.fori_loop(0, 4, send_near, 0)
    recv[me] = packed[me]

    count = jnp.zeros((32, LANES), F32)
    bits = jnp.zeros((32, LANES), F32)
    r_i, l_i = iota((LANES, LANES), 0), iota((LANES, LANES), 1)
    for a in range(8):
        m = mask_ref[pl.ds(a, 32, stride=8), :].astype(F32).astype(BF16)
        pool = jnp.where(l_i == 16 * a + r_i // K, 1.0, 0.0)
        weight = lax.shift_left(jnp.ones_like(r_i), r_i % K).astype(F32)
        count = count + dot(m, pool.astype(BF16))
        bits = bits + dot(m, (pool * weight).astype(BF16))
    first = dot(
        count.astype(BF16), ones_where((r_i < l_i) & (r_i // 64 == l_i // 64))
    ).astype(jnp.int32)
    load_assign.wait()
    to = assign_ref[...]
    source = 2 * iota((32, LANES), 0) + iota((32, LANES), 1) // 64
    quarter = lax.rem(lax.rem(to, 64) // 16 - first // QROWS + 8, 4)
    at = quarter * (N_SCEN * HELD) + source * HELD + lax.rem(first, QROWS)
    slots[0] = (to // 64).astype(F32)
    slots[1] = lax.rem(to, 64).astype(F32)
    slots[2] = (at // 256).astype(F32)
    slots[3] = lax.rem(at, 256).astype(F32)
    slots[4] = bits

    def place(k, acc):
        s_i = iota((64, LANES), 0).astype(F32)
        high = jnp.where(s_i == slots[0, pl.ds(k, 1), :], 1.0, 0.0)
        low = jnp.where(s_i == slots[1, pl.ds(k, 1), :], 1.0, 0.0).astype(BF16)
        return tuple(
            acc[j] + dot_nt((high * slots[2 + j, pl.ds(k, 1), :]).astype(BF16), low)
            for j in range(3)
        )

    zero = jnp.zeros((64, 64), F32)
    at_hi, at_lo, pattern = lax.fori_loop(0, 32, place, (zero, zero, zero))
    tbl_ref[...] = (at_hi * 256.0 + at_lo).astype(jnp.int32)
    k_i = lax.rem(iota((64, LANES), 1), K)
    for q in range(4):
        spread = ones_where(iota((64, LANES), 0) - 16 * q == iota((64, LANES), 1) // K)
        pat = dot(pattern.astype(BF16), spread).astype(jnp.int32)
        before_k = jnp.zeros((64, LANES), jnp.int32)
        own_bit = jnp.zeros((64, LANES), jnp.int32)
        for m in range(K):
            bit = lax.shift_right_logical(pat, m) & 1
            before_k = before_k + jnp.where(k_i > m, bit, 0)
            own_bit = own_bit + jnp.where(k_i == m, bit, 0)
        idx_ref[q] = iota((64, LANES), 1) - k_i + before_k
        val_ref[q] = own_bit.astype(F32)

    def take(s, acc):
        x = recv[s]
        tall = jnp.concatenate([x, pltpu.roll(x[:8], LANES - PART, 1)], axis=0)
        for p in range(4):
            y = pltpu.roll(tall, PART * p, 1) if p else tall
            turned[pl.ds(pl.multiple_of((p * N_SCEN + s) * HELD, 8), HELD), :] = y
        return acc + x * x

    def pass_on(k):
        j = ahead(k)
        to_relay(j).wait_recv()
        forward(j).start()

    def from_near(k, acc):
        s = zh * half + behind(k)
        arrival(s).wait_recv()
        return take(s, acc)

    def from_far(k, acc):
        s = (1 - zh) * half + behind(k)
        arrival(s).wait_recv()
        return take(s, acc)

    def early(k, acc):
        pass_on(k)
        return from_near(k, acc)

    def steady(k, acc):
        pass_on(k)
        return from_far(k - LAG, from_near(k, acc))

    acc = take(me, jnp.zeros((QROWS, LANES), F32))
    acc = lax.fori_loop(0, LAG, early, acc)
    acc = lax.fori_loop(LAG, last, steady, acc)
    acc = lax.fori_loop(last - LAG, half, from_far, acc)
    col = jnp.sum(acc, axis=0, keepdims=True)
    col = jnp.broadcast_to(col, (8, LANES))
    col = col + pltpu.roll(col, 64, 1)
    col = col + pltpu.roll(col, 32, 1)
    inv_ref[...] = 1.0 / jnp.sqrt(col / (ACT_DEV * N_SCEN) + EPS)

    def finish(j, _):
        to_relay(ahead(j)).wait_send()
        forward(ahead(j)).wait_send()
        direct(zh * half + ahead(j)).wait_send()
        return 0

    lax.fori_loop(0, last, finish, 0)
    direct(across).wait_send()


def place_kernel(per_step, tbl_ref, turned, inv_ref, idx_ref, val_ref, out_ref):
    step = pl.program_id(0)
    inv = inv_ref[...]
    lane_group = iota((8, LANES), 1) // PART

    for h in range(per_step):
        hi = step * per_step + h
        tiles = []
        for i in range(16):
            m = None
            for q in range(4):
                x = turned[pl.ds(tbl_ref[hi, 16 * q + i], 8), :]
                m = x if m is None else jnp.where(lane_group == q, x, m)
            tiles.append(m * inv)
        flipped = jnp.concatenate(tiles, axis=0).T
        for q in range(4):
            idx = jnp.broadcast_to(idx_ref[q, pl.ds(hi, 1), :], (PART, LANES))
            val = jnp.broadcast_to(val_ref[q, pl.ds(hi, 1), :], (PART, LANES))
            y = flipped[q * PART : (q + 1) * PART, :]
            y = jnp.take_along_axis(y, idx, axis=1) * val
            at = h * 512 + q * LANES
            out_ref[0, :, at : at + LANES] = y


def on_device(coef, mask, assign):
    rows, width = coef.shape
    vmem = pl.BlockSpec(memory_space=pltpu.VMEM)
    hbm = pl.BlockSpec(memory_space=pltpu.HBM)

    def in_hbm(x):
        return pltpu.with_memory_space_constraint(x, pltpu.HBM)

    turned, inv, tbl, idx, val = pl.pallas_call(
        exchange_kernel,
        out_shape=(
            pltpu.VMEM((4 * N_SCEN * HELD, LANES), F32),
            jax.ShapeDtypeStruct((8, LANES), F32),
            jax.ShapeDtypeStruct((64, 64), jnp.int32),
            jax.ShapeDtypeStruct((4, 64, LANES), jnp.int32),
            jax.ShapeDtypeStruct((4, 64, LANES), F32),
        ),
        in_specs=[hbm, hbm, hbm],
        out_specs=(vmem, vmem, vmem, vmem, vmem),
        scratch_shapes=[
            pltpu.VMEM((rows, width), F32),
            pltpu.VMEM((256, LANES), jnp.int32),
            pltpu.VMEM((32, LANES), jnp.int32),
            pltpu.VMEM((ACT_DEV, rows), BF16),
            pltpu.VMEM((ACT_DEV, width), F32),
            pltpu.VMEM((N_SCEN, QROWS, LANES), F32),
            pltpu.VMEM((N_SCEN // 2, QROWS, LANES), F32),
            pltpu.VMEM((N_SCEN, QROWS, LANES), F32),
            pltpu.VMEM((COLS, 8, ACT_DEV), F32),
            pltpu.VMEM((5, 32, LANES), F32),
            pltpu.SemaphoreType.DMA((2,)),
            pltpu.SemaphoreType.DMA((8,)),
            pltpu.SemaphoreType.DMA((COLS - 1,)),
            pltpu.SemaphoreType.DMA((COLS - 1,)),
            pltpu.SemaphoreType.REGULAR,
            pltpu.SemaphoreType.REGULAR,
            pltpu.SemaphoreType.DMA((N_SCEN,)),
            pltpu.SemaphoreType.DMA((N_SCEN,)),
            pltpu.SemaphoreType.DMA((N_SCEN // 2,)),
            pltpu.SemaphoreType.DMA((N_SCEN // 2,)),
        ],
        compiler_params=pltpu.CompilerParams(
            collective_id=0, has_side_effects=True, vmem_limit_bytes=20 * 2**20
        ),
        name="exchange",
    )(
        in_hbm(coef),
        in_hbm(mask.reshape(256, LANES)),
        in_hbm(assign.reshape(32, LANES)),
    )

    steps = 8
    per_step = 64 // steps

    def fixed(*shape):
        return pl.BlockSpec(shape, lambda i: (0,) * len(shape))

    return pl.pallas_call(
        functools.partial(place_kernel, per_step),
        out_shape=jax.ShapeDtypeStruct((1, PART, 64 * 512), F32),
        grid=(steps,),
        in_specs=[
            pl.BlockSpec(memory_space=pltpu.SMEM),
            vmem,
            fixed(8, LANES),
            fixed(4, 64, LANES),
            fixed(4, 64, LANES),
        ],
        out_specs=pl.BlockSpec((1, PART, per_step * 512), lambda i: (0, 0, i)),
        compiler_params=pltpu.CompilerParams(
            dimension_semantics=("arbitrary",), vmem_limit_bytes=16 * 2**20
        ),
        name="place",
    )(tbl, turned, inv, idx, val)


def solution(mesh):
    in_specs = (P("scen", "col"), P(), P())
    out_specs = P("col", "scen", None)
    return jax.shard_map(
        on_device, mesh=mesh, in_specs=in_specs, out_specs=out_specs, check_vma=False
    )
```

```python
import functools

import jax
import jax.numpy as jnp
from jax import lax
from jax.experimental import pallas as pl
from jax.experimental.pallas import tpu as pltpu
from jax.sharding import PartitionSpec as P

NV = 8192
K = 8
ACT_DEV = 256
EPS = 1e-06

LANES = 128
PART = 32
QROWS = 64
HELD = QROWS + 8
N_SCEN = 64
LAG = 4
COLS = 4
MESH = pl.DeviceIdType.MESH
F32 = jnp.float32
BF16 = jnp.bfloat16


def iota(shape, dim):
    return lax.broadcasted_iota(jnp.int32, shape, dim)


def ones_where(cond):
    return jnp.where(cond, 1.0, 0.0).astype(BF16)


def dot(a, b):
    return jnp.dot(a, b, preferred_element_type=F32)


def dot_nt(a, b):
    return lax.dot_general(
        a, b, (((1,), (1,)), ((), ())), preferred_element_type=F32
    )


def exchange_kernel(
    coef_ref,
    mask_hbm,
    assign_hbm,
    turned,
    inv_ref,
    tbl_ref,
    idx_ref,
    val_ref,
    coef_v,
    mask_ref,
    assign_ref,
    pick,
    dense,
    packed,
    relay,
    recv,
    part,
    slots,
    small_sem,
    in_sem,
    csend,
    crecv,
    axis_sem,
    twin_sem,
    ssem,
    rsem,
    relay_sem,
    forward_sem,
):
    rows, width = coef_ref.shape
    me = lax.axis_index("scen")
    group = lax.axis_index("col")
    half = N_SCEN // 2
    zh = me // half
    chunk = 256
    n_chunks = width // chunk

    def load(e):
        cols = pl.ds(pl.multiple_of(e * chunk, chunk), chunk)
        return pltpu.make_async_copy(
            coef_ref.at[:, cols], coef_v.at[:, cols], in_sem.at[e]
        )

    load_mask = pltpu.make_async_copy(mask_hbm, mask_ref, small_sem.at[0])
    load_assign = pltpu.make_async_copy(assign_hbm, assign_ref, small_sem.at[1])
    load_mask.start()
    for e in range(n_chunks):
        load(e).start()
    load_assign.start()

    own = me % half
    across = (me + half) % N_SCEN
    own_x, own_y, own_c = own // 8, own // 2 % 4, own % 2

    def index(x, y, c):
        return x % 4 * 8 + y % 4 * 2 + c % 2

    def signal(sem, device):
        pl.semaphore_signal(sem, inc=1, device_id=device, device_id_type=MESH)

    along_x = [{"scen": zh * half + index(own_x + d, own_y, own_c)} for d in (1, 2, 3)]
    along_y = [{"scen": zh * half + index(own_x, own_y + d, own_c)} for d in (1, 2, 3)]
    twin = {"scen": zh * half + index(own_x, own_y, own_c + 1)}
    others = [{"col": (group + d) % COLS} for d in range(1, COLS)]

    barrier = pltpu.get_barrier_semaphore()
    for device in [{"scen": across}] + others + along_x + along_y + [twin]:
        signal(barrier, device)

    load_mask.wait()

    mine = mask_ref[pl.ds(pl.multiple_of(me // 2 * 8, 8), 8), :].astype(F32)
    mine = jnp.where(me % 2 == 1, pltpu.roll(mine, 4, 0), mine)
    before = ones_where(iota((LANES, LANES), 0) < iota((LANES, LANES), 1))
    rank = dot(mine.astype(BF16), before)
    base = jnp.zeros((1, 1), F32)
    for k in range(rows // LANES):
        row = mine[k : k + 1, :]
        here = (rank[k : k + 1, :] + base).astype(jnp.int32)
        here = jnp.where(row > 0.5, here, -1)
        pick[:, k * LANES : (k + 1) * LANES] = ones_where(
            iota((ACT_DEV, LANES), 0) == here
        )
        base = base + jnp.sum(row, axis=1, keepdims=True)

    def compact(e, acc):
        load(e).wait()
        cols = pl.ds(pl.multiple_of(e * chunk, chunk), chunk)
        x = coef_v[:, cols]
        hi = x.astype(BF16)
        low = (x - hi.astype(F32)).astype(BF16)
        sel = pick[...]
        z = dot(sel, hi) + dot(sel, low)
        dense[:, cols] = z
        for j in range(chunk // LANES):
            zj = z[:, j * LANES : (j + 1) * LANES]
            acc = acc + zj * zj
        return acc

    acc = lax.fori_loop(0, n_chunks, compact, jnp.zeros((ACT_DEV, LANES), F32))
    sums = jnp.sum(acc.T, axis=0, keepdims=True)
    part[group] = jnp.broadcast_to(sums, (8, ACT_DEV))

    pl.semaphore_wait(barrier, 11)

    def share(d):
        return pltpu.make_async_remote_copy(
            src_ref=part.at[group],
            dst_ref=part.at[group],
            send_sem=csend.at[d - 1],
            recv_sem=crecv.at[d - 1],
            device_id={"col": (group + d) % COLS},
            device_id_type=MESH,
        )

    for d in range(1, COLS):
        share(d).start()
    for device in along_x + [twin]:
        signal(axis_sem, device)
    for d in range(1, COLS):
        share(d).wait()
    total = part[0] + part[1] + part[2] + part[3]
    inv_row = 1.0 / jnp.sqrt(total[0:1, :] / NV + EPS)
    scale = jnp.broadcast_to(inv_row, (LANES, ACT_DEV)).T

    lane_group = iota((QROWS, LANES), 1) // PART

    def pack(e):
        cols = pl.ds(pl.multiple_of(e * LANES, LANES), LANES)
        quarters = [
            dense[q * QROWS : (q + 1) * QROWS, cols]
            * scale[q * QROWS : (q + 1) * QROWS, :]
            for q in range(4)
        ]
        for f in range(4):
            out = None
            for q in range(4):
                shift = PART * (q - f) % LANES
                moved = pltpu.roll(quarters[q], shift, 1) if shift else quarters[q]
                out = moved if out is None else jnp.where(lane_group == q, moved, out)
            packed[4 * e + f] = out

    def offset(i):
        late = i // 2
        return (1 - late) * (2 - i) + late * (9 - 3 * i)

    def ahead(k):
        return index(
            own_x + offset(k // 8), own_y + offset(k // 2 % 4), own_c + 1 - k % 2
        )

    def behind(k):
        return index(
            own_x + 4 - offset(k // 8), own_y + 4 - offset(k // 2 % 4), own_c + 1 - k % 2
        )

    def to_relay(j):
        return pltpu.make_async_remote_copy(
            src_ref=packed.at[(1 - zh) * half + j],
            dst_ref=relay.at[j],
            send_sem=ssem.at[(1 - zh) * half + j],
            recv_sem=relay_sem.at[j],
            device_id={"scen": across},
            device_id_type=MESH,
        )

    def direct(d):
        return pltpu.make_async_remote_copy(
            src_ref=packed.at[d],
            dst_ref=recv.at[me],
            send_sem=ssem.at[d],
            recv_sem=rsem.at[me],
            device_id={"scen": d},
            device_id_type=MESH,
        )

    def forward(j):
        return pltpu.make_async_remote_copy(
            src_ref=relay.at[j],
            dst_ref=recv.at[across],
            send_sem=forward_sem.at[j],
            recv_sem=rsem.at[across],
            device_id={"scen": zh * half + j},
            device_id_type=MESH,
        )

    def arrival(s):
        return pltpu.make_async_remote_copy(
            src_ref=packed.at[s],
            dst_ref=recv.at[s],
            send_sem=ssem.at[s],
            recv_sem=rsem.at[s],
            device_id={"scen": s},
            device_id_type=MESH,
        )

    last = half - 1

    def send_far(i, _):
        x = (own_x + offset(i)) % 4
        for p in range(2):
            pack((1 - zh) * 8 + x * 2 + p)
        for j in range(8):
            k = 8 * i + j
            if j < 7:
                to_relay(ahead(k)).start()
            else:

                @pl.when(k < last)
                def _():
                    to_relay(ahead(k)).start()

        return 0

    lax.fori_loop(0, 4, send_far, 0)
    direct(across).start()

    pl.semaphore_wait(axis_sem, 4)
    signal(twin_sem, twin)
    pl.semaphore_wait(twin_sem, 1)

    def send_near(i, _):
        x = (own_x + offset(i)) % 4
        for p in range(2):
            pack(zh * 8 + x * 2 + p)
        for j in range(8):
            k = 8 * i + j
            if j < 7:
                direct(zh * half + ahead(k)).start()
            else:

                @pl.when(k < last)
                def _():
                    direct(zh * half + ahead(k)).start()

        return 0

    lax.fori_loop(0, 4, send_near, 0)
    recv[me] = packed[me]

    count = jnp.zeros((32, LANES), F32)
    bits = jnp.zeros((32, LANES), F32)
    r_i, l_i = iota((LANES, LANES), 0), iota((LANES, LANES), 1)
    for a in range(8):
        m = mask_ref[pl.ds(a, 32, stride=8), :].astype(F32).astype(BF16)
        pool = jnp.where(l_i == 16 * a + r_i // K, 1.0, 0.0)
        weight = lax.shift_left(jnp.ones_like(r_i), r_i % K).astype(F32)
        count = count + dot(m, pool.astype(BF16))
        bits = bits + dot(m, (pool * weight).astype(BF16))
    first = dot(
        count.astype(BF16), ones_where((r_i < l_i) & (r_i // 64 == l_i // 64))
    ).astype(jnp.int32)
    load_assign.wait()
    to = assign_ref[...]
    source = 2 * iota((32, LANES), 0) + iota((32, LANES), 1) // 64
    quarter = lax.rem(lax.rem(to, 64) // 16 - first // QROWS + 8, 4)
    at = quarter * (N_SCEN * HELD) + source * HELD + lax.rem(first, QROWS)
    slots[0] = (to // 64).astype(F32)
    slots[1] = lax.rem(to, 64).astype(F32)
    slots[2] = (at // 256).astype(F32)
    slots[3] = lax.rem(at, 256).astype(F32)
    slots[4] = bits

    def place(k, acc):
        s_i = iota((64, LANES), 0).astype(F32)
        high = jnp.where(s_i == slots[0, pl.ds(k, 1), :], 1.0, 0.0)
        low = jnp.where(s_i == slots[1, pl.ds(k, 1), :], 1.0, 0.0).astype(BF16)
        return tuple(
            acc[j] + dot_nt((high * slots[2 + j, pl.ds(k, 1), :]).astype(BF16), low)
            for j in range(3)
        )

    zero = jnp.zeros((64, 64), F32)
    at_hi, at_lo, pattern = lax.fori_loop(0, 32, place, (zero, zero, zero))
    tbl_ref[...] = (at_hi * 256.0 + at_lo).astype(jnp.int32)
    k_i = lax.rem(iota((64, LANES), 1), K)
    for q in range(4):
        spread = ones_where(iota((64, LANES), 0) - 16 * q == iota((64, LANES), 1) // K)
        pat = dot(pattern.astype(BF16), spread).astype(jnp.int32)
        before_k = jnp.zeros((64, LANES), jnp.int32)
        own_bit = jnp.zeros((64, LANES), jnp.int32)
        for m in range(K):
            bit = lax.shift_right_logical(pat, m) & 1
            before_k = before_k + jnp.where(k_i > m, bit, 0)
            own_bit = own_bit + jnp.where(k_i == m, bit, 0)
        idx_ref[q] = iota((64, LANES), 1) - k_i + before_k
        val_ref[q] = own_bit.astype(F32)

    def take(s, acc):
        x = recv[s]
        tall = jnp.concatenate([x, pltpu.roll(x[:8], LANES - PART, 1)], axis=0)
        for p in range(4):
            y = pltpu.roll(tall, PART * p, 1) if p else tall
            turned[pl.ds(pl.multiple_of((p * N_SCEN + s) * HELD, 8), HELD), :] = y
        return acc + x * x

    def pass_on(k):
        j = ahead(k)
        to_relay(j).wait_recv()
        forward(j).start()

    def from_near(k, acc):
        s = zh * half + behind(k)
        arrival(s).wait_recv()
        return take(s, acc)

    def from_far(k, acc):
        s = (1 - zh) * half + behind(k)
        arrival(s).wait_recv()
        return take(s, acc)

    def early(k, acc):
        pass_on(k)
        return from_near(k, acc)

    def steady(k, acc):
        pass_on(k)
        return from_far(k - LAG, from_near(k, acc))

    acc = take(me, jnp.zeros((QROWS, LANES), F32))
    acc = lax.fori_loop(0, LAG, early, acc)
    acc = lax.fori_loop(LAG, last, steady, acc)
    acc = lax.fori_loop(last - LAG, half, from_far, acc)
    col = jnp.sum(acc, axis=0, keepdims=True)
    col = jnp.broadcast_to(col, (8, LANES))
    col = col + pltpu.roll(col, 64, 1)
    col = col + pltpu.roll(col, 32, 1)
    inv_ref[...] = 1.0 / jnp.sqrt(col / (ACT_DEV * N_SCEN) + EPS)

    def finish(j, _):
        to_relay(ahead(j)).wait_send()
        forward(ahead(j)).wait_send()
        direct(zh * half + ahead(j)).wait_send()
        return 0

    lax.fori_loop(0, last, finish, 0)
    direct(across).wait_send()


def place_kernel(per_step, tbl_ref, turned, inv_ref, idx_ref, val_ref, out_ref):
    step = pl.program_id(0)
    inv = inv_ref[...]
    lane_group = iota((8, LANES), 1) // PART

    for h in range(per_step):
        hi = step * per_step + h
        tiles = []
        for i in range(16):
            m = None
            for q in range(4):
                x = turned[pl.ds(tbl_ref[hi, 16 * q + i], 8), :]
                m = x if m is None else jnp.where(lane_group == q, x, m)
            tiles.append(m * inv)
        flipped = jnp.concatenate(tiles, axis=0).T
        for q in range(4):
            idx = jnp.broadcast_to(idx_ref[q, pl.ds(hi, 1), :], (PART, LANES))
            val = jnp.broadcast_to(val_ref[q, pl.ds(hi, 1), :], (PART, LANES))
            y = flipped[q * PART : (q + 1) * PART, :]
            y = jnp.take_along_axis(y, idx, axis=1) * val
            at = h * 512 + q * LANES
            out_ref[0, :, at : at + LANES] = y


def on_device(coef, mask, assign):
    rows, width = coef.shape
    vmem = pl.BlockSpec(memory_space=pltpu.VMEM)
    hbm = pl.BlockSpec(memory_space=pltpu.HBM)

    def in_hbm(x):
        return pltpu.with_memory_space_constraint(x, pltpu.HBM)

    turned, inv, tbl, idx, val = pl.pallas_call(
        exchange_kernel,
        out_shape=(
            pltpu.VMEM((4 * N_SCEN * HELD, LANES), F32),
            jax.ShapeDtypeStruct((8, LANES), F32),
            jax.ShapeDtypeStruct((64, 64), jnp.int32),
            jax.ShapeDtypeStruct((4, 64, LANES), jnp.int32),
            jax.ShapeDtypeStruct((4, 64, LANES), F32),
        ),
        in_specs=[hbm, hbm, hbm],
        out_specs=(vmem, vmem, vmem, vmem, vmem),
        scratch_shapes=[
            pltpu.VMEM((rows, width), F32),
            pltpu.VMEM((256, LANES), jnp.int32),
            pltpu.VMEM((32, LANES), jnp.int32),
            pltpu.VMEM((ACT_DEV, rows), BF16),
            pltpu.VMEM((ACT_DEV, width), F32),
            pltpu.VMEM((N_SCEN, QROWS, LANES), F32),
            pltpu.VMEM((N_SCEN // 2, QROWS, LANES), F32),
            pltpu.VMEM((N_SCEN, QROWS, LANES), F32),
            pltpu.VMEM((COLS, 8, ACT_DEV), F32),
            pltpu.VMEM((5, 32, LANES), F32),
            pltpu.SemaphoreType.DMA((2,)),
            pltpu.SemaphoreType.DMA((8,)),
            pltpu.SemaphoreType.DMA((COLS - 1,)),
            pltpu.SemaphoreType.DMA((COLS - 1,)),
            pltpu.SemaphoreType.REGULAR,
            pltpu.SemaphoreType.REGULAR,
            pltpu.SemaphoreType.DMA((N_SCEN,)),
            pltpu.SemaphoreType.DMA((N_SCEN,)),
            pltpu.SemaphoreType.DMA((N_SCEN // 2,)),
            pltpu.SemaphoreType.DMA((N_SCEN // 2,)),
        ],
        compiler_params=pltpu.CompilerParams(
            collective_id=0, has_side_effects=True, vmem_limit_bytes=20 * 2**20
        ),
        name="exchange",
    )(
        in_hbm(coef),
        in_hbm(mask.reshape(256, LANES)),
        in_hbm(assign.reshape(32, LANES)),
    )

    steps = 4
    per_step = 64 // steps

    def fixed(*shape):
        return pl.BlockSpec(shape, lambda i: (0,) * len(shape))

    return pl.pallas_call(
        functools.partial(place_kernel, per_step),
        out_shape=jax.ShapeDtypeStruct((1, PART, 64 * 512), F32),
        grid=(steps,),
        in_specs=[
            pl.BlockSpec(memory_space=pltpu.SMEM),
            vmem,
            fixed(8, LANES),
            fixed(4, 64, LANES),
            fixed(4, 64, LANES),
        ],
        out_specs=pl.BlockSpec((1, PART, per_step * 512), lambda i: (0, 0, i)),
        compiler_params=pltpu.CompilerParams(
            dimension_semantics=("arbitrary",), vmem_limit_bytes=16 * 2**20
        ),
        name="place",
    )(tbl, turned, inv, idx, val)


def solution(mesh):
    in_specs = (P("scen", "col"), P(), P())
    out_specs = P("col", "scen", None)
    return jax.shard_map(
        on_device, mesh=mesh, in_specs=in_specs, out_specs=out_specs, check_vma=False
    )
```
